32 devices in a mesh: replica: 1 (over z), ep: 32 (over y, x, core).
Axes of the slice: x: 4, y: 4, z: 1, core: 2. Of those that a mesh axis runs over, the one named last changes fastest.
The devices are a block of a 4x4x8 slice.
Arguments:
- tok_in: bfloat16 [2048, 1536], P(('replica', 'ep'))
- routes: int32 [2, 2048, 6], P(None, ('replica', 'ep'))
- gate_vals: float32 [2, 2048, 6], P(None, ('replica', 'ep'))
- w_gate: bfloat16 [2, 64, 1536, 512], P(None, ('replica', 'ep'))
- w_up: bfloat16 [2, 64, 1536, 512], P(None, ('replica', 'ep'))
- w_down: bfloat16 [2, 64, 512, 1536], P(None, ('replica', 'ep'))
- sh_gate: bfloat16 [2, 1536, 1024], replicated
- sh_up: bfloat16 [2, 1536, 1024], replicated
- sh_down: bfloat16 [2, 1024, 1536], replicated
- old_map: int32 [2, 64], P(None, 'replica')
- move_slot: int32 [2, 2], P(None, 'replica')
- move_expert: int32 [2, 2], P(None, 'replica')
Outputs:
- output 1: bfloat16 [2048, 1536], P(('replica', 'ep'))
- output 2: bfloat16 [2, 64, 1536, 512], P(None, ('replica', 'ep'))
- output 3: bfloat16 [2, 64, 1536, 512], P(None, ('replica', 'ep'))
- output 4: bfloat16 [2, 64, 512, 1536], P(None, ('replica', 'ep'))
All inputs are finite; a program needn't handle non-finite values.
Results may differ from the reference program's by a relative error of at most 0.011583.
Values are sent between devices in bfloat16 or wider.
A program may use at most 768 MiB of HBM per device.

```python
import jax
import jax.numpy as jnp
from jax import lax

HIDDEN = 1536
EXPERT_FF = 512
SHARED_FF = 1024
TOP_K = 6
GROUP_DEVS = 32
SLOTS_DEV = 2
TOKENS_DEV = 64
MOVE_COUNT = 2
EXPERTS = 51

SLOT_COUNT = GROUP_DEVS * SLOTS_DEV
TOKEN_COUNT = GROUP_DEVS * TOKENS_DEV
SCORE_RANGE = 2 ** 10
HOT_BONUS = 2 ** 9
COVER_BONUS = 2 ** 12


def draw_layout(rng_key):
    perm_key, extra_key, place_key = jax.random.split(rng_key, 3)
    expert_perm = jax.random.permutation(perm_key, EXPERTS).astype(jnp.int32)
    extra_slot = jax.random.randint(extra_key, (SLOT_COUNT - EXPERTS,), 0, EXPERTS, dtype=jnp.int32)
    canon_old = jnp.concatenate([expert_perm, extra_slot])
    cycled = jnp.concatenate([expert_perm[1:MOVE_COUNT], expert_perm[:1]])
    slot_perm = jax.random.permutation(place_key, SLOT_COUNT).astype(jnp.int32)
    old_map = canon_old[slot_perm]
    slot_of_canon = jnp.argsort(slot_perm).astype(jnp.int32)
    return old_map, slot_of_canon[:MOVE_COUNT], cycled, expert_perm[:MOVE_COUNT]


def draw_routes(rng_key, hot_ids):
    score_key, offset_key = jax.random.split(rng_key)
    score_int = jax.random.randint(score_key, (TOKEN_COUNT, EXPERTS), 0, SCORE_RANGE, dtype=jnp.int32)
    expert_ids = jnp.arange(EXPERTS, dtype=jnp.int32)
    is_hot = jnp.any(expert_ids[:, None] == hot_ids[None, :], axis=1).astype(jnp.int32)
    offset = jax.random.randint(offset_key, (), 0, EXPERTS, dtype=jnp.int32)
    token_ids = jnp.arange(TOKEN_COUNT, dtype=jnp.int32)
    cover_mask = ((token_ids[:, None] + offset) % EXPERTS == expert_ids[None, :]).astype(jnp.int32)
    total_score = score_int + HOT_BONUS * is_hot[None, :] + COVER_BONUS * cover_mask
    picked = lax.top_k(total_score * EXPERTS + expert_ids[None, :], TOP_K)[1]
    return picked.astype(jnp.int32)


def place_slots(expert_w, slot_map):
    return jnp.take(expert_w, slot_map, axis=0)


def setup_inputs(seed: int = 0, part: int = 0) -> dict:
    base_key = jax.random.key(seed)
    part_key = jax.random.fold_in(base_key, part)
    draw_keys = jax.random.split(part_key, 7)
    shared_keys = jax.random.split(jax.random.key(seed + 1), 3)
    old_map, move_slot, move_expert, hot_ids = jax.vmap(draw_layout)(jax.random.split(draw_keys[0], 2))
    routes = jax.vmap(draw_routes)(jax.random.split(draw_keys[1], 2), hot_ids)
    gate_vals = (0.5 + jax.random.uniform(draw_keys[2], (2, TOKEN_COUNT, TOP_K))) / TOP_K ** 0.5
    tok_in = jax.random.normal(draw_keys[3], (TOKEN_COUNT, HIDDEN)).astype(jnp.bfloat16)
    gate_e = (jax.random.normal(draw_keys[4], (2, EXPERTS, HIDDEN, EXPERT_FF)) * HIDDEN ** -0.5).astype(jnp.bfloat16)
    up_e = (jax.random.normal(draw_keys[5], (2, EXPERTS, HIDDEN, EXPERT_FF)) * HIDDEN ** -0.5).astype(jnp.bfloat16)
    down_e = (jax.random.normal(draw_keys[6], (2, EXPERTS, EXPERT_FF, HIDDEN)) * EXPERT_FF ** -0.5).astype(jnp.bfloat16)
    sh_gate = (jax.random.normal(shared_keys[0], (2, HIDDEN, SHARED_FF)) * HIDDEN ** -0.5).astype(jnp.bfloat16)
    sh_up = (jax.random.normal(shared_keys[1], (2, HIDDEN, SHARED_FF)) * HIDDEN ** -0.5).astype(jnp.bfloat16)
    sh_down = (jax.random.normal(shared_keys[2], (2, SHARED_FF, HIDDEN)) * SHARED_FF ** -0.5).astype(jnp.bfloat16)
    return {
        'tok_in': tok_in,
        'routes': routes,
        'gate_vals': gate_vals,
        'w_gate': jax.vmap(place_slots)(gate_e, old_map),
        'w_up': jax.vmap(place_slots)(up_e, old_map),
        'w_down': jax.vmap(place_slots)(down_e, old_map),
        'sh_gate': sh_gate,
        'sh_up': sh_up,
        'sh_down': sh_down,
        'old_map': old_map,
        'move_slot': move_slot,
        'move_expert': move_expert,
    }


def first_holder(slot_map, wanted):
    slot_ids = jnp.arange(SLOT_COUNT, dtype=jnp.int32)
    hit_mask = slot_map[None, :] == wanted[:, None]
    return jnp.min(jnp.where(hit_mask, slot_ids[None, :], SLOT_COUNT), axis=1)


def swiglu(hidden, w_gate, w_up, w_down):
    gate_proj = jnp.dot(hidden, w_gate, preferred_element_type=jnp.float32)
    up_proj = jnp.dot(hidden, w_up, preferred_element_type=jnp.float32)
    inner_act = (jax.nn.silu(gate_proj) * up_proj).astype(jnp.bfloat16)
    return jnp.dot(inner_act, w_down, preferred_element_type=jnp.float32)


def moe_layer(hidden, route_ids, gate_w, w_gate, w_up, w_down, sh_gate, sh_up, sh_down, slot_map):
    expert_ids = jnp.arange(EXPERTS, dtype=jnp.int32)
    holders = first_holder(slot_map, expert_ids)

    def add_expert(running, expert_idx):
        holder_slot = holders[expert_idx]
        expert_out = swiglu(hidden, w_gate[holder_slot], w_up[holder_slot], w_down[holder_slot])
        gate_col = jnp.sum(jnp.where(route_ids == expert_idx, gate_w, 0.0), axis=1)
        return running + gate_col[:, None] * expert_out, None

    start_acc = hidden.astype(jnp.float32) + swiglu(hidden, sh_gate, sh_up, sh_down)
    total_out = lax.scan(add_expert, start_acc, expert_ids)[0]
    return total_out.astype(jnp.bfloat16)


def reference(tok_in, routes, gate_vals, w_gate, w_up, w_down, sh_gate, sh_up, sh_down, old_map, move_slot, move_expert):
    hidden = tok_in
    new_sets = []
    for layer_idx in range(2):
        hidden = moe_layer(hidden, routes[layer_idx], gate_vals[layer_idx], w_gate[layer_idx], w_up[layer_idx], w_down[layer_idx], sh_gate[layer_idx], sh_up[layer_idx], sh_down[layer_idx], old_map[layer_idx])
        new_map = old_map[layer_idx].at[move_slot[layer_idx]].set(move_expert[layer_idx])
        source = first_holder(old_map[layer_idx], new_map)
        new_sets.append((jnp.take(w_gate[layer_idx], source, axis=0), jnp.take(w_up[layer_idx], source, axis=0), jnp.take(w_down[layer_idx], source, axis=0)))
    new_gate = jnp.stack([new_sets[0][0], new_sets[1][0]])
    new_up = jnp.stack([new_sets[0][1], new_sets[1][1]])
    new_down = jnp.stack([new_sets[0][2], new_sets[1][2]])
    return (hidden, new_gate, new_up, new_down)
```

```python
import functools

import jax
import jax.numpy as jnp
from jax import lax
from jax.experimental import pallas as pl
from jax.experimental.pallas import tpu as pltpu
from jax.sharding import PartitionSpec as P

TOKEN_AXES = ('replica', 'ep')
MESH = pl.DeviceIdType.MESH
F32 = jnp.float32
BF16 = jnp.bfloat16


def first_holder(slot_map, wanted):
    slot_ids = jnp.arange(slot_map.shape[0], dtype=jnp.int32)
    hit_mask = slot_map[None, :] == wanted[:, None]
    return jnp.min(jnp.where(hit_mask, slot_ids[None, :], slot_map.shape[0]), axis=1)


def send_moved(weights, slot_map, move_expert, slots_dev, my_dev):
    source = first_holder(slot_map, move_expert)
    is_source = (source // slots_dev) == my_dev
    local_idx = source % slots_dev
    return tuple(jnp.where(is_source[:, None, None], jnp.take(weight_arr, local_idx, axis=0), jnp.zeros((), weight_arr.dtype)) for weight_arr in weights)


def place_moved(weights, arrived, move_slot, slots_dev, my_dev):
    local_ids = my_dev * slots_dev + jnp.arange(slots_dev, dtype=jnp.int32)
    match_mask = (move_slot[None, :] == local_ids[:, None]).astype(jnp.int32)
    is_target = jnp.max(match_mask, axis=1) > 0
    pick_idx = jnp.argmax(match_mask, axis=1)
    return tuple(jnp.where(is_target[:, None, None], jnp.take(arrived_arr, pick_idx, axis=0), weight_arr) for arrived_arr, weight_arr in zip(arrived, weights))


def gate_table(routes, gate_vals, old_map):
    cols = []
    slot_ids = jnp.arange(old_map.shape[1], dtype=jnp.int32)
    for layer in range(old_map.shape[0]):
        serve = first_holder(old_map[layer], old_map[layer]) == slot_ids
        hit = (routes[layer][:, :, None] == old_map[layer][None, None, :]) & serve[None, None, :]
        cols.append(jnp.sum(jnp.where(hit, gate_vals[layer][:, :, None], 0.0), axis=1))
    return jnp.concatenate(cols, axis=1)


def moe_kernel(side, tok, coef, wg, wu, wd, sg, su, sd, out,
               xb, cb, wgv, wuv, wdv, sgv, suv, sdv, act, hacc, own, pcs, pcr, rs,
               wsem, ssem, tsem, xsend, xrecv, msend, mrecv, csend, crecv, cmsend, cmrecv,
               psend, precv, rsend, rrecv, mid):
    layers, slots, dim, ff = wg.shape
    rows = tok.shape[0]
    half = rows // 2
    n = side * side
    me = lax.axis_index('ep')
    core = lax.rem(me, 2)
    chip = lax.div(me, 2)
    yy = lax.div(chip, side)
    xx = lax.rem(chip, side)
    ga = yy * (1 - core) + xx * core
    gb = xx * (1 - core) + yy * core
    pos = side * ga + lax.rem(ga + gb, side)

    def ring_dev(k):
        k = lax.rem(k, n)
        a = lax.div(k, side)
        b = lax.rem(lax.rem(k, side) - a + side, side)
        y = a * (1 - core) + b * core
        x = b * (1 - core) + a * core
        return (y * side + x) * 2 + core

    peers = (ring_dev(pos + 1), ring_dev(pos + n - 1))
    mate = me + 1 - 2 * core

    def remote(src, dst, ss, rr, dev):
        return pltpu.make_async_remote_copy(src_ref=src, dst_ref=dst, send_sem=ss, recv_sem=rr,
                                            device_id={'ep': dev}, device_id_type=MESH)

    def part(d):
        return pl.ds(d * half, half)

    mine, theirs = pl.ds(0, rows), pl.ds(rows, rows)

    def xcopy(l, s, d):
        return remote(xb.at[l, s, part(d)], xb.at[l, s + 1, part(d)], xsend.at[l, s, d], xrecv.at[l, s + 1, d], peers[d])

    def mcopy(l, s):
        return remote(xb.at[l, s, mine], xb.at[l, s, theirs], msend.at[l, s], mrecv.at[l, s], mate)

    def ccopy(s, d):
        return remote(cb.at[s, part(d)], cb.at[s + 1, part(d)], csend.at[s, d], crecv.at[s + 1, d], peers[d])

    def cmcopy(s):
        return remote(cb.at[s, mine], cb.at[s, theirs], cmsend.at[s], cmrecv.at[s], mate)

    def pcopy(l, s):
        return remote(pcs.at[lax.rem(s, 2)], pcr.at[s], psend.at[lax.rem(s, 2)], precv.at[l, s], mate)

    def rcopy(l, s, d):
        return remote(rs.at[s, part(d)], rs.at[s + 1, part(d)], rsend.at[l, s, d], rrecv.at[l, s + 1, d], peers[d])

    def shared_loads(l):
        return [pltpu.make_async_copy(src.at[l], dst, ssem.at[l, i]) for i, (src, dst) in enumerate(((sg, sgv), (su, suv), (sd, sdv)))]

    def expert_loads(l):
        return [pltpu.make_async_copy(src.at[l], dst.at[l], wsem.at[l, i]) for i, (src, dst) in enumerate(((wg, wgv), (wu, wuv), (wd, wdv)))]

    tok_in = pltpu.make_async_copy(tok, xb.at[0, 0, mine], tsem.at[0])
    coef_in = pltpu.make_async_copy(coef, cb.at[0, mine], tsem.at[1])
    tok_in.start()
    coef_in.start()
    for copy in shared_loads(0):
        copy.start()
    for l in range(layers):
        for copy in expert_loads(l):
            copy.start()

    barrier = pltpu.get_barrier_semaphore()
    for dev in peers + (mate,):
        pl.semaphore_signal(barrier, inc=1, device_id={'ep': dev}, device_id_type=MESH)
    pl.semaphore_wait(barrier, 3)
    tok_in.wait()
    coef_in.wait()

    def forward(l, s):
        for d in range(2):
            xcopy(l, s, d).start()
            if l == 0:
                ccopy(s, d).start()

    def to_mate(l, s):
        mcopy(l, s).start()
        if l == 0:
            cmcopy(s).start()

    def wait_block(l, s):
        for d in range(2):
            xcopy(l, s - 1, d).wait_recv()
            if l == 0:
                ccopy(s - 1, d).wait_recv()

    def wait_mate(l, s):
        mcopy(l, s).wait_recv()
        if l == 0:
            cmcopy(s).wait_recv()

    fblk = min(ff, 256)
    dblk = min(dim, 512)

    def experts(l, s):
        x = xb.at[l, s]
        table = cb[s]
        lane = lax.broadcasted_iota(jnp.int32, table.shape, 1)
        weight = []
        for i in range(slots):
            col = l * (coef.shape[1] // layers) + me * slots + i
            weight.append(jnp.sum(jnp.where(lane == col, table, 0.0), axis=1, keepdims=True))
            for f in range(0, ff, fblk):
                g = jnp.dot(x[...], wgv[l, i, :, f:f + fblk], preferred_element_type=F32)
                u = jnp.dot(x[...], wuv[l, i, :, f:f + fblk], preferred_element_type=F32)
                act[i, :, f:f + fblk] = (jax.nn.silu(g) * u).astype(BF16)
        slot = lax.rem(s, 2)
        for c in range(0, dim, dblk):
            total = None
            for i in range(slots):
                o = jnp.dot(act[i], wdv[l, i, :, c:c + dblk], preferred_element_type=F32) * weight[i]
                total = o if total is None else total + o
            own[:, c:c + dblk] = total[:rows]
            pcs[slot, :, c:c + dblk] = total[rows:]

    for l in range(layers):
        forward(l, 0)
        to_mate(l, 0)
        if l > 0:
            drain(l - 1)
            for dev in peers + (mate,):
                pl.semaphore_signal(mid, inc=1, device_id={'ep': dev}, device_id_type=MESH)
        for copy in shared_loads(l):
            copy.wait()
        h = xb.at[l, 0, mine]
        sff = sgv.shape[1]
        for f in range(0, sff, fblk):
            g = jnp.dot(h[...], sgv[:, f:f + fblk], preferred_element_type=F32)
            u = jnp.dot(h[...], suv[:, f:f + fblk], preferred_element_type=F32)
            act_sh = (jax.nn.silu(g) * u).astype(BF16)
            act[f // ff, 0:rows, f % ff:f % ff + fblk] = act_sh
        for c in range(0, dim, dblk):
            total = h[:, c:c + dblk].astype(F32)
            for f in range(0, sff, ff):
                w = min(ff, sff - f)
                total = total + jnp.dot(act[f // ff, 0:rows, 0:w], sdv[f:f + w, c:c + dblk], preferred_element_type=F32)
            hacc[:, c:c + dblk] = total
        if l + 1 < layers:
            for copy in shared_loads(l + 1):
                copy.start()
        for copy in expert_loads(l):
            copy.wait()
        if l > 0:
            pl.semaphore_wait(mid, 3)
        wait_mate(l, 0)
        experts(l, 0)
        pcopy(l, 0).start()
        hacc[...] += own[...]
        wait_block(l, 1)
        forward(l, 1)
        to_mate(l, 1)

        def step(s, carry):
            wait_mate(l, s)

            @pl.when(s >= 2)
            def _():
                pcopy(l, s - 2).wait_send()

            experts(l, s)
            pcopy(l, s).start()

            @pl.when(s < n - 1)
            def _():
                wait_block(l, s + 1)
                to_mate(l, s + 1)

            @pl.when(s < n - 2)
            def _():
                forward(l, s + 1)

            pcopy(l, s).wait_recv()

            @pl.when(s == 1)
            def _():
                rs[s] = own[...] + pcr[s]

            @pl.when(s > 1)
            def _():
                for d in range(2):
                    rcopy(l, s - 1, d).wait_recv()
                rs[s] = rs[s] + (own[...] + pcr[s])

            for d in range(2):
                rcopy(l, s, d).start()
            return carry

        lax.fori_loop(1, n, step, 0)
        for d in range(2):
            rcopy(l, n - 1, d).wait_recv()
        pcopy(l, 0).wait_recv()
        new_h = (hacc[...] + (pcr[0] + rs[n])).astype(BF16)
        if l + 1 < layers:
            xb[l + 1, 0, mine] = new_h
        else:
            out[...] = new_h

        def drain(l):
            pcopy(l, n - 2).wait_send()
            pcopy(l, n - 1).wait_send()
            mcopy(l, 0).wait_send()
            if l == 0:
                cmcopy(0).wait_send()
            for d in range(2):
                xcopy(l, 0, d).wait_send()
                if l == 0:
                    ccopy(0, d).wait_send()

            def one(s, carry):
                mcopy(l, s).wait_send()
                if l == 0:
                    cmcopy(s).wait_send()
                for d in range(2):
                    rcopy(l, s, d).wait_send()

                @pl.when(s < n - 1)
                def _():
                    for d in range(2):
                        xcopy(l, s, d).wait_send()
                        if l == 0:
                            ccopy(s, d).wait_send()
                return carry

            lax.fori_loop(1, n, one, 0)

    drain(layers - 1)


def moe(tok, coef, wg, wu, wd, sg, su, sd, group):
    layers, slots, dim, ff = wg.shape
    rows = tok.shape[0]
    sff = sg.shape[2]
    n = group // 2
    side = int(round(n ** 0.5))
    assert side * side * 2 == group
    dma = pltpu.SemaphoreType.DMA
    any_spec = pl.BlockSpec(memory_space=pl.ANY)
    vmem = pltpu.VMEM
    act_n = max(slots, -(-sff // ff))
    scratch = [
        vmem((layers, n, 2 * rows, dim), BF16),
        vmem((n, 2 * rows, coef.shape[1]), F32),
        vmem((layers, slots, dim, ff), BF16),
        vmem((layers, slots, dim, ff), BF16),
        vmem((layers, slots, ff, dim), BF16),
        vmem((dim, sff), BF16),
        vmem((dim, sff), BF16),
        vmem((sff, dim), BF16),
        vmem((act_n, 2 * rows, ff), BF16),
        vmem((rows, dim), F32),
        vmem((rows, dim), F32),
        vmem((2, rows, dim), F32),
        vmem((n, rows, dim), F32),
        vmem((n + 1, rows, dim), F32),
        dma((layers, 3)), dma((layers, 3)), dma((2,)),
        dma((layers, n, 2)), dma((layers, n, 2)),
        dma((layers, n)), dma((layers, n)),
        dma((n, 2)), dma((n, 2)),
        dma((n,)), dma((n,)),
        dma((2,)), dma((layers, n)),
        dma((layers, n, 2)), dma((layers, n + 1, 2)),
        pltpu.SemaphoreType.REGULAR,
    ]
    flops = layers * 2 * 3 * dim * (ff * slots * rows * group + sff * rows)
    return pl.pallas_call(
        functools.partial(moe_kernel, side),
        out_shape=jax.ShapeDtypeStruct((rows, dim), BF16),
        in_specs=[any_spec] * 8,
        out_specs=pl.BlockSpec(memory_space=pltpu.VMEM),
        scratch_shapes=scratch,
        compiler_params=pltpu.CompilerParams(collective_id=0, has_side_effects=True, vmem_limit_bytes=67043328),
        cost_estimate=pl.CostEstimate(flops=flops * 4, bytes_accessed=40 << 20, transcendentals=0),
        name='moe_rings',
    )(tok, coef, wg, wu, wd, sg, su, sd)


def solution(mesh):
    group = mesh.shape['ep']

    def body(tok_in, routes, gate_vals, w_gate, w_up, w_down, sh_gate, sh_up, sh_down, old_map, move_slot, move_expert):
        my_dev = lax.axis_index('ep')
        layers, slots_dev = w_gate.shape[:2]
        placed = []
        for layer in range(layers):
            layer_w = (w_gate[layer], w_up[layer], w_down[layer])
            outgoing = send_moved(layer_w, old_map[layer], move_expert[layer], slots_dev, my_dev)
            arrived = lax.psum(outgoing, 'ep')
            placed.append(place_moved(layer_w, arrived, move_slot[layer], slots_dev, my_dev))
        coef = gate_table(routes, gate_vals, old_map)
        hidden = moe(tok_in, coef, w_gate, w_up, w_down, sh_gate, sh_up, sh_down, group)
        new_w = tuple(jnp.stack([p[i] for p in placed]) for i in range(3))
        return (hidden,) + new_w

    weight_spec = P(None, TOKEN_AXES, None, None)
    route_spec = P(None, TOKEN_AXES, None)
    map_spec = P(None, 'replica')
    shared_spec = P(None, None, None)
    tok_spec = P(TOKEN_AXES, None)
    return jax.shard_map(body, mesh=mesh, in_specs=(tok_spec, route_spec, route_spec, weight_spec, weight_spec, weight_spec, shared_spec, shared_spec, shared_spec, map_spec, map_spec, map_spec), out_specs=(tok_spec, weight_spec, weight_spec, weight_spec), check_vma=False)
```

```python
import functools

import jax
import jax.numpy as jnp
from jax import lax
from jax.experimental import pallas as pl
from jax.experimental.pallas import tpu as pltpu
from jax.sharding import PartitionSpec as P

TOKEN_AXES = ('replica', 'ep')
MESH = pl.DeviceIdType.MESH
F32 = jnp.float32
BF16 = jnp.bfloat16


def first_holder(slot_map, wanted):
    slot_ids = jnp.arange(slot_map.shape[0], dtype=jnp.int32)
    hit_mask = slot_map[None, :] == wanted[:, None]
    return jnp.min(jnp.where(hit_mask, slot_ids[None, :], slot_map.shape[0]), axis=1)


def gate_table(routes, gate_vals, old_map):
    cols = []
    slot_ids = jnp.arange(old_map.shape[1], dtype=jnp.int32)
    for layer in range(old_map.shape[0]):
        serve = first_holder(old_map[layer], old_map[layer]) == slot_ids
        hit = (routes[layer][:, :, None] == old_map[layer][None, None, :]) & serve[None, None, :]
        cols.append(jnp.sum(jnp.where(hit, gate_vals[layer][:, :, None], 0.0), axis=1))
    return jnp.concatenate(cols, axis=1)


SUB = 32
CELLS = 4


def unit_counts(dim, ff):
    per_block, blocks = ff // 4 // SUB, dim // ff
    return per_block, blocks, 3 * blocks * per_block


def moe_kernel(side, src, tok, coef, wg, wu, wd, sg, su, sd, out, hist,
               cell, obuf, cin, cout, xb, cb, wgv, wuv, wdv, sgv, suv, sdv, act, hacc, own, pcs, pcr, rs,
               wsem, ssem, tsem, xsend, xrecv, msend, mrecv, csend, crecv, cmsend, cmrecv,
               psend, precv, rsend, rrecv,
               osend, orecv, hsend, hlocal, hrecv, vsend, vrecv, cred, vcred, mid):
    layers, slots, dim, ff = wg.shape
    rows = tok.shape[0]
    half = rows // 2
    n = side * side
    me = lax.axis_index('ep')
    core = lax.rem(me, 2)
    chip = lax.div(me, 2)
    yy = lax.div(chip, side)
    xx = lax.rem(chip, side)
    ga = yy * (1 - core) + xx * core
    gb = xx * (1 - core) + yy * core
    pos = side * ga + lax.rem(ga + gb, side)

    def ring_dev(k):
        k = lax.rem(k, n)
        a = lax.div(k, side)
        b = lax.rem(lax.rem(k, side) - a + side, side)
        y = a * (1 - core) + b * core
        x = b * (1 - core) + a * core
        return (y * side + x) * 2 + core

    peers = (ring_dev(pos + 1), ring_dev(pos + n - 1))
    mate = me + 1 - 2 * core

    def remote(src, dst, ss, rr, dev):
        return pltpu.make_async_remote_copy(src_ref=src, dst_ref=dst, send_sem=ss, recv_sem=rr,
                                            device_id={'ep': dev}, device_id_type=MESH)

    def part(d):
        return pl.ds(d * half, half)

    mine, theirs = pl.ds(0, rows), pl.ds(rows, rows)

    def xcopy(l, s, d):
        return remote(xb.at[l, s, part(d)], xb.at[l, s + 1, part(d)], xsend.at[l, s, d], xrecv.at[l, s + 1, d], peers[d])

    def mcopy(l, s):
        return remote(xb.at[l, s, mine], xb.at[l, s, theirs], msend.at[l, s], mrecv.at[l, s], mate)

    def ccopy(s, d):
        return remote(cb.at[s, part(d)], cb.at[s + 1, part(d)], csend.at[s, d], crecv.at[s + 1, d], peers[d])

    def cmcopy(s):
        return remote(cb.at[s, mine], cb.at[s, theirs], cmsend.at[s], cmrecv.at[s], mate)

    def pcopy(l, s):
        return remote(pcs.at[lax.rem(s, 2)], pcr.at[s], psend.at[lax.rem(s, 2)], precv.at[l, s], mate)

    def rcopy(l, s, d):
        return remote(rs.at[s, part(d)], rs.at[s + 1, part(d)], rsend.at[l, s, d], rrecv.at[l, s + 1, d], peers[d])

    per_block, blocks, units = unit_counts(dim, ff)
    per_matrix = blocks * per_block
    total_moves = src.shape[0]
    per_layer = total_moves // layers
    trips = units + n - 1
    quarter = ff // 4

    def ocopy(t, d):
        return remote(obuf.at[lax.rem(t, 2), d], cell.at[lax.rem(t, CELLS), d], osend.at[lax.rem(t, 2), d], orecv.at[lax.rem(t, CELLS), d], peers[d])

    def hcopy(t):
        return remote(cell.at[lax.rem(t, CELLS)], hist.at[1, t], hsend.at[lax.rem(t, 2)], hrecv.at[t], mate)

    def hkeep(t):
        return pltpu.make_async_copy(cell.at[lax.rem(t, CELLS)], hist.at[0, t], hlocal.at[lax.rem(t, 2)])

    def vcopy(t):
        return remote(cout.at[lax.rem(t, 2)], cin.at[lax.rem(t, 2)], vsend.at[lax.rem(t, 2)], vrecv.at[lax.rem(t, 2)], mate)

    def own_piece(m, t, mv, q):
        j = t - m * per_matrix
        b = lax.div(j, per_block)
        r = q * quarter + lax.rem(j, per_block) * SUB
        l = mv // per_layer
        val = None
        for i in range(slots):
            if m < 2:
                new = (wgv, wuv)[m][l, i, pl.ds(pl.multiple_of(b * ff + r, SUB), SUB), :]
            else:
                new = wdv[l, i, pl.ds(pl.multiple_of(r, SUB), SUB), pl.ds(pl.multiple_of(b * ff, ff), ff)]
            val = new if val is None else jnp.where(src[mv] == me * slots + i, new, val)
        return val

    def by_matrix(t, fn):
        for m in range(3):
            @pl.when((t >= m * per_matrix) & (t < (m + 1) * per_matrix))
            def _():
                fn(m)

    def offer(t):
        slot = lax.rem(t, 2)

        @pl.when(t >= 2)
        def _():
            vcopy(t - 2).wait_send()
            pl.semaphore_wait(vcred, 1)

        def fill(m):
            for d in range(2):
                for mv in range(total_moves):
                    cout[slot, d, mv] = own_piece(m, t, mv, 2 * (1 - core) + d)

        by_matrix(t, fill)
        vcopy(t).start()

    def convey(t):
        last = lax.rem(t + CELLS - 1, CELLS)
        slot = lax.rem(t, 2)

        @pl.when((t >= 2) & (t <= trips + 1))
        def _():
            hkeep(t - 2).wait()
            hcopy(t - 2).wait_send()

        @pl.when((t >= 1) & (t <= trips + 1 - CELLS))
        def _():
            for d in range(2):
                pl.semaphore_signal(cred.at[d], inc=1, device_id={'ep': peers[1 - d]}, device_id_type=MESH)

        @pl.when((t >= 1) & (t <= trips))
        def _():
            for d in range(2):
                ocopy(t - 1, d).wait_recv()
            hkeep(t - 1).start()
            hcopy(t - 1).start()

        @pl.when(t < trips)
        def _():
            @pl.when(t >= CELLS - 1)
            def _():
                for d in range(2):
                    pl.semaphore_wait(cred.at[d], 1)

            @pl.when(t >= 2)
            def _():
                for d in range(2):
                    ocopy(t - 2, d).wait_send()

            @pl.when(t < units)
            def _():
                vcopy(t).wait_recv()

                def fill(m):
                    for d in range(2):
                        for mv in range(total_moves):
                            holder = lax.div(src[mv], slots)
                            val = jnp.where(holder == mate, cin[slot, d, mv], cell[last, d, mv])
                            obuf[slot, d, mv] = jnp.where(holder == me, own_piece(m, t, mv, 2 * core + d), val)

                by_matrix(t, fill)

                @pl.when(t < units - 2)
                def _():
                    pl.semaphore_signal(vcred, inc=1, device_id={'ep': mate}, device_id_type=MESH)

            @pl.when(t >= units)
            def _():
                obuf[slot] = cell[last]

            for d in range(2):
                ocopy(t, d).start()

            @pl.when(t + 1 < units)
            def _():
                offer(t + 1)

    def shared_loads(l):
        return [pltpu.make_async_copy(src.at[l], dst, ssem.at[l, i]) for i, (src, dst) in enumerate(((sg, sgv), (su, suv), (sd, sdv)))]

    def expert_loads(l):
        return [pltpu.make_async_copy(src.at[l], dst.at[l], wsem.at[l, i]) for i, (src, dst) in enumerate(((wg, wgv), (wu, wuv), (wd, wdv)))]

    tok_in = pltpu.make_async_copy(tok, xb.at[0, 0, mine], tsem.at[0])
    coef_in = pltpu.make_async_copy(coef, cb.at[0, mine], tsem.at[1])
    tok_in.start()
    coef_in.start()
    for copy in shared_loads(0):
        copy.start()
    for l in range(layers):
        for copy in expert_loads(l):
            copy.start()

    cell[CELLS - 1] = jnp.zeros(cell.shape[1:], cell.dtype)

    barrier = pltpu.get_barrier_semaphore()
    for dev in peers + (mate,):
        pl.semaphore_signal(barrier, inc=1, device_id={'ep': dev}, device_id_type=MESH)
    pl.semaphore_wait(barrier, 3)
    tok_in.wait()
    coef_in.wait()

    def forward(l, s):
        for d in range(2):
            xcopy(l, s, d).start()
            if l == 0:
                ccopy(s, d).start()

    def to_mate(l, s):
        mcopy(l, s).start()
        if l == 0:
            cmcopy(s).start()

    def wait_block(l, s):
        for d in range(2):
            xcopy(l, s - 1, d).wait_recv()
            if l == 0:
                ccopy(s - 1, d).wait_recv()

    def wait_mate(l, s):
        mcopy(l, s).wait_recv()
        if l == 0:
            cmcopy(s).wait_recv()

    fblk = min(ff, 256)
    dblk = min(dim, 512)

    def experts(l, s):
        x = xb.at[l, s]
        table = cb[s]
        lane = lax.broadcasted_iota(jnp.int32, table.shape, 1)
        weight = []
        for i in range(slots):
            col = l * (coef.shape[1] // layers) + me * slots + i
            weight.append(jnp.sum(jnp.where(lane == col, table, 0.0), axis=1, keepdims=True))
            for f in range(0, ff, fblk):
                g = jnp.dot(x[...], wgv[l, i, :, f:f + fblk], preferred_element_type=F32)
                u = jnp.dot(x[...], wuv[l, i, :, f:f + fblk], preferred_element_type=F32)
                act[i, :, f:f + fblk] = (jax.nn.silu(g) * u).astype(BF16)
        slot = lax.rem(s, 2)
        for c in range(0, dim, dblk):
            total = None
            for i in range(slots):
                o = jnp.dot(act[i], wdv[l, i, :, c:c + dblk], preferred_element_type=F32) * weight[i]
                total = o if total is None else total + o
            own[:, c:c + dblk] = total[:rows]
            pcs[slot, :, c:c + dblk] = total[rows:]

    for l in range(layers):
        forward(l, 0)
        to_mate(l, 0)
        if l > 0:
            drain(l - 1)
            for dev in peers + (mate,):
                pl.semaphore_signal(mid, inc=1, device_id={'ep': dev}, device_id_type=MESH)
        for copy in shared_loads(l):
            copy.wait()
        h = xb.at[l, 0, mine]
        sff = sgv.shape[1]
        for f in range(0, sff, fblk):
            g = jnp.dot(h[...], sgv[:, f:f + fblk], preferred_element_type=F32)
            u = jnp.dot(h[...], suv[:, f:f + fblk], preferred_element_type=F32)
            act_sh = (jax.nn.silu(g) * u).astype(BF16)
            act[f // ff, 0:rows, f % ff:f % ff + fblk] = act_sh
        for c in range(0, dim, dblk):
            total = h[:, c:c + dblk].astype(F32)
            for f in range(0, sff, ff):
                w = min(ff, sff - f)
                total = total + jnp.dot(act[f // ff, 0:rows, 0:w], sdv[f:f + w, c:c + dblk], preferred_element_type=F32)
            hacc[:, c:c + dblk] = total
        if l + 1 < layers:
            for copy in shared_loads(l + 1):
                copy.start()
        if l == 0:
            for k in range(layers):
                for copy in expert_loads(k):
                    copy.wait()
            offer(0)
        if l > 0:
            pl.semaphore_wait(mid, 3)
        wait_mate(l, 0)
        experts(l, 0)
        pcopy(l, 0).start()
        hacc[...] += own[...]
        wait_block(l, 1)
        forward(l, 1)
        to_mate(l, 1)

        def step(s, carry):
            trip = 2 * (l * (n - 1) + s - 1)
            convey(trip)
            wait_mate(l, s)

            @pl.when(s >= 2)
            def _():
                pcopy(l, s - 2).wait_send()

            experts(l, s)
            pcopy(l, s).start()

            @pl.when(s < n - 1)
            def _():
                wait_block(l, s + 1)
                to_mate(l, s + 1)

            @pl.when(s < n - 2)
            def _():
                forward(l, s + 1)

            convey(trip + 1)
            pcopy(l, s).wait_recv()

            @pl.when(s == 1)
            def _():
                rs[s] = own[...] + pcr[s]

            @pl.when(s > 1)
            def _():
                for d in range(2):
                    rcopy(l, s - 1, d).wait_recv()
                rs[s] = rs[s] + (own[...] + pcr[s])

            for d in range(2):
                rcopy(l, s, d).start()
            return carry

        lax.fori_loop(1, n, step, 0)
        for d in range(2):
            rcopy(l, n - 1, d).wait_recv()
        pcopy(l, 0).wait_recv()
        new_h = (hacc[...] + (pcr[0] + rs[n])).astype(BF16)
        if l + 1 < layers:
            xb[l + 1, 0, mine] = new_h
        else:
            out[...] = new_h

        def drain(l):
            pcopy(l, n - 2).wait_send()
            pcopy(l, n - 1).wait_send()
            mcopy(l, 0).wait_send()
            if l == 0:
                cmcopy(0).wait_send()
            for d in range(2):
                xcopy(l, 0, d).wait_send()
                if l == 0:
                    ccopy(0, d).wait_send()

            def one(s, carry):
                mcopy(l, s).wait_send()
                if l == 0:
                    cmcopy(s).wait_send()
                for d in range(2):
                    rcopy(l, s, d).wait_send()

                @pl.when(s < n - 1)
                def _():
                    for d in range(2):
                        xcopy(l, s, d).wait_send()
                        if l == 0:
                            ccopy(s, d).wait_send()
                return carry

            lax.fori_loop(1, n, one, 0)

    drain(layers - 1)
    for t in (trips - 2, trips - 1):
        for d in range(2):
            ocopy(t, d).wait_send()
    for t in (units - 2, units - 1):
        vcopy(t).wait_send()

    def landed(t, carry):
        hcopy(t).wait_recv()
        return carry

    lax.fori_loop(0, trips, landed, 0)


def place_kernel(side, src, slot_to, hist, wg, wu, wd, og, ou, od, bg, bu, bd, rsem, wsem):
    layers, slots = wg.shape[:2]
    n = side * side
    per_layer = src.shape[0] // layers
    ff = hist.shape[-1]
    per_block = ff // 4 // SUB
    blocks = wg.shape[2] // (4 * per_block)
    me = lax.axis_index('ep')

    def place(dev):
        chip = lax.div(dev, 2)
        y, x = lax.div(chip, side), lax.rem(chip, side)
        turn = lax.rem(x + y, side)
        return side * y + turn, side * x + turn

    core = lax.rem(me, 2)
    at = place(me)
    groups = tuple(zip((wg, wu, wd), (bg, bu, bd), (og, ou, od)))
    for l in range(layers):
        for i in range(slots):
            here = me * slots + i
            moved = slot_to[l * per_layer] == here
            mv = l * per_layer
            for k in range(1, per_layer):
                hit = slot_to[l * per_layer + k] == here
                moved = moved | hit
                mv = jnp.where(hit, l * per_layer + k, mv)
            origin = place(lax.div(src[mv], slots))

            @pl.when(jnp.logical_not(moved))
            def _():
                for m, (w, buf, _) in enumerate(groups):
                    pltpu.make_async_copy(w.at[l, i], buf.at[l, i], rsem.at[l, i, m]).start()

            @pl.when(moved)
            def _():
                for which in range(2):
                    ring = core if which == 0 else 1 - core
                    gap = (at[0] - origin[0]) * (1 - ring) + (at[1] - origin[1]) * ring
                    for d in range(2):
                        away = lax.rem((gap if d == 0 else -gap) - 1 + 2 * n, n)
                        for m, (_, buf, _) in enumerate(groups):
                            for b in range(blocks):
                                first = away + (m * blocks + b) * per_block
                                come = hist.at[which, pl.ds(first, per_block), d, mv]
                                q = (2 * ring + d) * per_block
                                if m < 2:
                                    dst = buf.at[l, i, pl.ds(b * 4 * per_block + q, per_block)]
                                else:
                                    dst = buf.at[l, i, pl.ds(q, per_block), :, pl.ds(b * ff, ff)]
                                pltpu.make_async_copy(come, dst, rsem.at[l, i, m]).start()

    for l in range(layers):
        for i in range(slots):
            for m, (w, buf, o) in enumerate(groups):
                pltpu.make_async_copy(w.at[l, i], buf.at[l, i], rsem.at[l, i, m]).wait()
                pltpu.make_async_copy(buf.at[l, i], o.at[l, i], wsem.at[l, i, m]).start()
    for l in range(layers):
        for i in range(slots):
            for m, (w, buf, o) in enumerate(groups):
                pltpu.make_async_copy(buf.at[l, i], o.at[l, i], wsem.at[l, i, m]).wait()


def place_weights(src, slot_to, hist, weights, side):
    layers, slots = weights[0].shape[:2]
    split = [w.reshape(layers, slots, w.shape[2] // SUB, SUB, w.shape[3]) for w in weights]
    any_spec = pl.BlockSpec(memory_space=pl.ANY)
    smem = pl.BlockSpec(memory_space=pltpu.SMEM)
    out = pl.pallas_call(
        functools.partial(place_kernel, side),
        out_shape=[jax.ShapeDtypeStruct(w.shape, w.dtype) for w in split],
        in_specs=[smem, smem] + [any_spec] * 4,
        out_specs=[any_spec] * 3,
        scratch_shapes=[pltpu.VMEM(w.shape, w.dtype) for w in split] + [pltpu.SemaphoreType.DMA((layers, slots, 3))] * 2,
        compiler_params=pltpu.CompilerParams(vmem_limit_bytes=40 << 20),
        name='place_slots',
    )(src, slot_to, hist, *split)
    return tuple(o.reshape(w.shape) for o, w in zip(out, weights))


def moe(src, tok, coef, wg, wu, wd, sg, su, sd, group):
    layers, slots, dim, ff = wg.shape
    rows = tok.shape[0]
    sff = sg.shape[2]
    n = group // 2
    side = int(round(n ** 0.5))
    assert side * side * 2 == group
    dma = pltpu.SemaphoreType.DMA
    any_spec = pl.BlockSpec(memory_space=pl.ANY)
    vmem = pltpu.VMEM
    act_n = max(slots, -(-sff // ff))
    per_block, blocks, units = unit_counts(dim, ff)
    trips = units + n - 1
    moves = src.shape[0]
    assert 2 * layers * (n - 1) > trips + 1 and units > 2
    piece = (2, moves, SUB, ff)
    scratch = [
        vmem((CELLS,) + piece, BF16),
        vmem((2,) + piece, BF16),
        vmem((2,) + piece, BF16),
        vmem((2,) + piece, BF16),
        vmem((layers, n, 2 * rows, dim), BF16),
        vmem((n, 2 * rows, coef.shape[1]), F32),
        vmem((layers, slots, dim, ff), BF16),
        vmem((layers, slots, dim, ff), BF16),
        vmem((layers, slots, ff, dim), BF16),
        vmem((dim, sff), BF16),
        vmem((dim, sff), BF16),
        vmem((sff, dim), BF16),
        vmem((act_n, 2 * rows, ff), BF16),
        vmem((rows, dim), F32),
        vmem((rows, dim), F32),
        vmem((2, rows, dim), F32),
        vmem((n, rows, dim), F32),
        vmem((n + 1, rows, dim), F32),
        dma((layers, 3)), dma((layers, 3)), dma((2,)),
        dma((layers, n, 2)), dma((layers, n, 2)),
        dma((layers, n)), dma((layers, n)),
        dma((n, 2)), dma((n, 2)),
        dma((n,)), dma((n,)),
        dma((2,)), dma((layers, n)),
        dma((layers, n, 2)), dma((layers, n + 1, 2)),
        dma((2, 2)), dma((CELLS, 2)), dma((2,)), dma((2,)), dma((trips,)), dma((2,)), dma((2,)),
        pltpu.SemaphoreType.REGULAR((2,)), pltpu.SemaphoreType.REGULAR,
        pltpu.SemaphoreType.REGULAR,
    ]
    flops = layers * 2 * 3 * dim * (ff * slots * rows * group + sff * rows)
    return pl.pallas_call(
        functools.partial(moe_kernel, side),
        out_shape=[jax.ShapeDtypeStruct((rows, dim), BF16), jax.ShapeDtypeStruct((2, trips) + piece, BF16)],
        in_specs=[pl.BlockSpec(memory_space=pltpu.SMEM)] + [any_spec] * 8,
        out_specs=[pl.BlockSpec(memory_space=pltpu.VMEM), any_spec],
        scratch_shapes=scratch,
        compiler_params=pltpu.CompilerParams(collective_id=0, has_side_effects=True, vmem_limit_bytes=67043328),
        cost_estimate=pl.CostEstimate(flops=flops * 4, bytes_accessed=40 << 20, transcendentals=0),
        name='moe_rings',
    )(src, tok, coef, wg, wu, wd, sg, su, sd)


def solution(mesh):
    group = mesh.shape['ep']

    def body(tok_in, routes, gate_vals, w_gate, w_up, w_down, sh_gate, sh_up, sh_down, old_map, move_slot, move_expert):
        layers = w_gate.shape[0]
        src = jnp.concatenate([first_holder(old_map[l], move_expert[l]) for l in range(layers)])
        coef = gate_table(routes, gate_vals, old_map)
        hidden, hist = moe(src, tok_in, coef, w_gate, w_up, w_down, sh_gate, sh_up, sh_down, group)
        side = int(round((group // 2) ** 0.5))
        new_w = place_weights(src, move_slot.reshape(-1), hist, (w_gate, w_up, w_down), side)
        return (hidden,) + new_w

    weight_spec = P(None, TOKEN_AXES, None, None)
    route_spec = P(None, TOKEN_AXES, None)
    map_spec = P(None, 'replica')
    shared_spec = P(None, None, None)
    tok_spec = P(TOKEN_AXES, None)
    return jax.shard_map(body, mesh=mesh, in_specs=(tok_spec, route_spec, route_spec, weight_spec, weight_spec, weight_spec, shared_spec, shared_spec, shared_spec, map_spec, map_spec, map_spec), out_specs=(tok_spec, weight_spec, weight_spec, weight_spec), check_vma=False)
```

```python
import functools

import jax
import jax.numpy as jnp
from jax import lax
from jax.experimental import pallas as pl
from jax.experimental.pallas import tpu as pltpu
from jax.sharding import PartitionSpec as P

TOKEN_AXES = ('replica', 'ep')
MESH = pl.DeviceIdType.MESH
F32 = jnp.float32
BF16 = jnp.bfloat16


def first_holder(slot_map, wanted):
    slot_ids = jnp.arange(slot_map.shape[0], dtype=jnp.int32)
    hit_mask = slot_map[None, :] == wanted[:, None]
    return jnp.min(jnp.where(hit_mask, slot_ids[None, :], slot_map.shape[0]), axis=1)


def gate_table(routes, gate_vals, old_map):
    cols = []
    slot_ids = jnp.arange(old_map.shape[1], dtype=jnp.int32)
    for layer in range(old_map.shape[0]):
        serve = first_holder(old_map[layer], old_map[layer]) == slot_ids
        hit = (routes[layer][:, :, None] == old_map[layer][None, None, :]) & serve[None, None, :]
        cols.append(jnp.sum(jnp.where(hit, gate_vals[layer][:, :, None], 0.0), axis=1))
    return jnp.concatenate(cols, axis=1)


CELLS = 4
SUM_PARTS = 4
MOVE_PARTS = 4
TOK_PARTS = 2


def piece_rows(ff):
    return max(ff // 8, 32)


def unit_counts(dim, ff):
    per_block, blocks = ff // 4 // piece_rows(ff), dim // ff
    return per_block, blocks, 3 * blocks * per_block


def moe_kernel(side, src, tok, coef, wg, wu, wd, sg, su, sd, out, hist,
               cell, obuf, cin, cout, xb, cb, wgv, wuv, wdv, sgv, suv, sdv, act, hacc, own, pcs, pcr, rs,
               wsem, ssem, tsem, xsend, xrecv, msend, mrecv, csend, crecv, cmsend, cmrecv,
               psend, precv, rsend, rrecv,
               osend, orecv, hsend, hlocal, hrecv, vsend, vrecv, cred, vcred, mid):
    layers, slots, dim, ff = wg.shape
    rows = tok.shape[0]
    half = rows // 2
    n = side * side
    me = lax.axis_index('ep')
    core = lax.rem(me, 2)
    chip = lax.div(me, 2)
    yy = lax.div(chip, side)
    xx = lax.rem(chip, side)
    ga = yy * (1 - core) + xx * core
    gb = xx * (1 - core) + yy * core
    pos = side * ga + lax.rem(ga + gb, side)

    def ring_dev(k):
        k = lax.rem(k, n)
        a = lax.div(k, side)
        b = lax.rem(lax.rem(k, side) - a + side, side)
        y = a * (1 - core) + b * core
        x = b * (1 - core) + a * core
        return (y * side + x) * 2 + core

    peers = (ring_dev(pos + 1), ring_dev(pos + n - 1))
    mate = me + 1 - 2 * core

    def remote(src, dst, ss, rr, dev):
        return pltpu.make_async_remote_copy(src_ref=src, dst_ref=dst, send_sem=ss, recv_sem=rr,
                                            device_id={'ep': dev}, device_id_type=MESH)

    def part(d):
        return pl.ds(d * half, half)

    mine, theirs = pl.ds(0, rows), pl.ds(rows, rows)

    bit = half // TOK_PARTS

    def xcopy(l, s, d, p):
        r = pl.ds(d * half + p * bit, bit)
        return remote(xb.at[l, s, r], xb.at[l, s + 1, r], xsend.at[l, s, d, p], xrecv.at[l, s + 1, d, p], peers[d])

    def mcopy(l, s):
        return remote(xb.at[l, s, mine], xb.at[l, s, theirs], msend.at[l, s], mrecv.at[l, s], mate)

    def ccopy(s, d):
        return remote(cb.at[s, part(d)], cb.at[s + 1, part(d)], csend.at[s, d], crecv.at[s + 1, d], peers[d])

    def cmcopy(s):
        return remote(cb.at[s, mine], cb.at[s, theirs], cmsend.at[s], cmrecv.at[s], mate)

    def pcopy(l, s):
        return remote(pcs.at[lax.rem(s, 2)], pcr.at[s], psend.at[lax.rem(s, 2)], precv.at[l, s], mate)

    strip = half // SUM_PARTS

    def strips(p):
        return [pl.ds(d * half + p * strip, strip) for d in range(2)]

    def rcopy(l, s, d, p):
        rows_p = strips(p)[d]
        return remote(rs.at[s, rows_p], rs.at[s + 1, rows_p], rsend.at[l, s, d, p], rrecv.at[l, s + 1, d, p], peers[d])

    per_block, blocks, units = unit_counts(dim, ff)
    SUB = piece_rows(ff)
    per_matrix = blocks * per_block
    total_moves = src.shape[0]
    per_layer = total_moves // layers
    trips = units + n - 1
    quarter = ff // 4

    some = total_moves // MOVE_PARTS

    def ocopy(t, d, h):
        o, c, ms = lax.rem(t, 2), lax.rem(t, CELLS), pl.ds(h * some, some)
        return remote(obuf.at[o, d, ms], cell.at[c, d, ms], osend.at[o, d, h], orecv.at[c, d, h], peers[d])

    def hcopy(t):
        return remote(cell.at[lax.rem(t, CELLS)], hist.at[1, t], hsend.at[lax.rem(t, 2)], hrecv.at[t], mate)

    def hkeep(t):
        return pltpu.make_async_copy(cell.at[lax.rem(t, CELLS)], hist.at[0, t], hlocal.at[lax.rem(t, 2)])

    def vcopy(t):
        return remote(cout.at[lax.rem(t, 2)], cin.at[lax.rem(t, 2)], vsend.at[lax.rem(t, 2)], vrecv.at[lax.rem(t, 2)], mate)

    def own_piece(m, t, mv, q):
        j = t - m * per_matrix
        b = lax.div(j, per_block)
        r = q * quarter + lax.rem(j, per_block) * SUB
        l = mv // per_layer
        val = None
        for i in range(slots):
            if m < 2:
                new = (wgv, wuv)[m][l, i, pl.ds(pl.multiple_of(b * ff + r, SUB), SUB), :]
            else:
                new = wdv[l, i, pl.ds(pl.multiple_of(r, SUB), SUB), pl.ds(pl.multiple_of(b * ff, ff), ff)]
            val = new if val is None else jnp.where(src[mv] == me * slots + i, new, val)
        return val

    def by_matrix(t, fn):
        for m in range(3):
            @pl.when((t >= m * per_matrix) & (t < (m + 1) * per_matrix))
            def _():
                fn(m)

    def offer(t):
        slot = lax.rem(t, 2)

        @pl.when(t >= 2)
        def _():
            vcopy(t - 2).wait_send()
            pl.semaphore_wait(vcred, 1)

        def fill(m):
            for d in range(2):
                for mv in range(total_moves):
                    cout[slot, d, mv] = own_piece(m, t, mv, 2 * (1 - core) + d)

        by_matrix(t, fill)
        vcopy(t).start()

    def convey(t, between=None):
        last = lax.rem(t + CELLS - 1, CELLS)
        slot = lax.rem(t, 2)

        @pl.when((t >= 2) & (t <= trips + 1))
        def _():
            hkeep(t - 2).wait()
            hcopy(t - 2).wait_send()

        @pl.when((t >= 1) & (t <= trips + 1 - CELLS))
        def _():
            for d in range(2):
                pl.semaphore_signal(cred.at[d], inc=1, device_id={'ep': peers[1 - d]}, device_id_type=MESH)

        @pl.when(t < trips)
        def _():
            @pl.when(t >= CELLS - 1)
            def _():
                for d in range(2):
                    pl.semaphore_wait(cred.at[d], 1)

            @pl.when(t >= 2)
            def _():
                for d in range(2):
                    for h in range(MOVE_PARTS):
                        ocopy(t - 2, d, h).wait_send()

            @pl.when(t < units)
            def _():
                vcopy(t).wait_recv()

        for h in range(MOVE_PARTS):
            @pl.when((t >= 1) & (t <= trips))
            def _():
                for d in range(2):
                    ocopy(t - 1, d, h).wait_recv()

            def fill(m):
                for d in range(2):
                    for mv in range(h * some, (h + 1) * some):
                        holder = lax.div(src[mv], slots)
                        val = jnp.where(holder == mate, cin[slot, d, mv], cell[last, d, mv])
                        obuf[slot, d, mv] = jnp.where(holder == me, own_piece(m, t, mv, 2 * core + d), val)

            by_matrix(t, fill)

            @pl.when((t >= units) & (t < trips))
            def _():
                for d in range(2):
                    for mv in range(h * some, (h + 1) * some):
                        obuf[slot, d, mv] = cell[last, d, mv]

            @pl.when(t < trips)
            def _():
                for d in range(2):
                    ocopy(t, d, h).start()

            if between is not None:
                between(h)

        @pl.when((t >= 1) & (t <= trips))
        def _():
            hkeep(t - 1).start()
            hcopy(t - 1).start()

        @pl.when(t < units - 2)
        def _():
            pl.semaphore_signal(vcred, inc=1, device_id={'ep': mate}, device_id_type=MESH)

        @pl.when(t + 1 < units)
        def _():
            offer(t + 1)

    def shared_loads(l):
        return [pltpu.make_async_copy(src.at[l], dst, ssem.at[l, i]) for i, (src, dst) in enumerate(((sg, sgv), (su, suv), (sd, sdv)))]

    def expert_loads(l):
        return [pltpu.make_async_copy(src.at[l], dst.at[l], wsem.at[l, i]) for i, (src, dst) in enumerate(((wg, wgv), (wu, wuv), (wd, wdv)))]

    tok_in = pltpu.make_async_copy(tok, xb.at[0, 0, mine], tsem.at[0])
    coef_in = pltpu.make_async_copy(coef, cb.at[0, mine], tsem.at[1])
    tok_in.start()
    coef_in.start()
    for copy in shared_loads(0):
        copy.start()
    for l in range(layers):
        for copy in expert_loads(l):
            copy.start()

    cell[CELLS - 1] = jnp.zeros(cell.shape[1:], cell.dtype)

    barrier = pltpu.get_barrier_semaphore()
    for dev in peers + (mate,):
        pl.semaphore_signal(barrier, inc=1, device_id={'ep': dev}, device_id_type=MESH)
    pl.semaphore_wait(barrier, 3)
    tok_in.wait()
    coef_in.wait()

    def forward(l, s, p):
        for d in range(2):
            xcopy(l, s, d, p).start()
            if l == 0 and p == TOK_PARTS - 1:
                ccopy(s, d).start()

    def to_mate(l, s):
        mcopy(l, s).start()
        if l == 0:
            cmcopy(s).start()

    def wait_block(l, s, p):
        for d in range(2):
            xcopy(l, s - 1, d, p).wait_recv()
            if l == 0 and p == TOK_PARTS - 1:
                ccopy(s - 1, d).wait_recv()

    def wait_mate(l, s):
        mcopy(l, s).wait_recv()
        if l == 0:
            cmcopy(s).wait_recv()

    fblk = min(ff, 256)
    dblk = min(dim, 512)

    def experts(l, s):
        x = xb.at[l, s]
        table = cb[s]
        lane = lax.broadcasted_iota(jnp.int32, table.shape, 1)
        weight = []
        for i in range(slots):
            col = l * (coef.shape[1] // layers) + me * slots + i
            weight.append(jnp.sum(jnp.where(lane == col, table, 0.0), axis=1, keepdims=True))
            for f in range(0, ff, fblk):
                g = jnp.dot(x[...], wgv[l, i, :, f:f + fblk], preferred_element_type=F32)
                u = jnp.dot(x[...], wuv[l, i, :, f:f + fblk], preferred_element_type=F32)
                act[i, :, f:f + fblk] = (jax.nn.silu(g) * u).astype(BF16)
        slot = lax.rem(s, 2)
        for c in range(0, dim, dblk):
            total = None
            for i in range(slots):
                o = jnp.dot(act[i], wdv[l, i, :, c:c + dblk], preferred_element_type=F32) * weight[i]
                total = o if total is None else total + o
            own[:, c:c + dblk] = total[:rows]
            pcs[slot, :, c:c + dblk] = total[rows:]

    for l in range(layers):
        for p in range(TOK_PARTS):
            forward(l, 0, p)
        to_mate(l, 0)
        if l > 0:
            drain(l - 1)
            for dev in peers + (mate,):
                pl.semaphore_signal(mid, inc=1, device_id={'ep': dev}, device_id_type=MESH)
        for copy in shared_loads(l):
            copy.wait()
        h = xb.at[l, 0, mine]
        sff = sgv.shape[1]
        for f in range(0, sff, fblk):
            g = jnp.dot(h[...], sgv[:, f:f + fblk], preferred_element_type=F32)
            u = jnp.dot(h[...], suv[:, f:f + fblk], preferred_element_type=F32)
            act_sh = (jax.nn.silu(g) * u).astype(BF16)
            act[f // ff, 0:rows, f % ff:f % ff + fblk] = act_sh
        for c in range(0, dim, dblk):
            total = h[:, c:c + dblk].astype(F32)
            for f in range(0, sff, ff):
                w = min(ff, sff - f)
                total = total + jnp.dot(act[f // ff, 0:rows, 0:w], sdv[f:f + w, c:c + dblk], preferred_element_type=F32)
            hacc[:, c:c + dblk] = total
        if l + 1 < layers:
            for copy in shared_loads(l + 1):
                copy.start()
        if l == 0:
            for k in range(layers):
                for copy in expert_loads(k):
                    copy.wait()
            offer(0)
        if l > 0:
            pl.semaphore_wait(mid, 3)
        first_trip = l * (n + 2)
        convey(jnp.int32(first_trip))
        wait_mate(l, 0)
        experts(l, 0)
        pcopy(l, 0).start()
        hacc[...] += own[...]
        for p in range(TOK_PARTS):
            wait_block(l, 1, p)
            forward(l, 1, p)
        to_mate(l, 1)
        convey(jnp.int32(first_trip + 1))

        def step(s, carry):
            def come(p):
                @pl.when(s < n - 1)
                def _():
                    wait_block(l, s + 1, p)

                @pl.when(s < n - 2)
                def _():
                    forward(l, s + 1, p)

            def send_sums(h):
                if h == 0:
                    pcopy(l, s).wait_recv()
                for p in range(h * SUM_PARTS // MOVE_PARTS, (h + 1) * SUM_PARTS // MOVE_PARTS):
                    @pl.when(s == 1)
                    def _():
                        for r in strips(p):
                            rs[s, r] = own[r] + pcr[s, r]

                    @pl.when(s > 1)
                    def _():
                        for d in range(2):
                            rcopy(l, s - 1, d, p).wait_recv()
                        for r in strips(p):
                            rs[s, r] = rs[s, r] + (own[r] + pcr[s, r])

                    for d in range(2):
                        rcopy(l, s, d, p).start()

            wait_mate(l, s)
            for p in range(TOK_PARTS - 1):
                come(p)

            @pl.when(s >= 2)
            def _():
                pcopy(l, s - 2).wait_send()

            experts(l, s)
            pcopy(l, s).start()
            come(TOK_PARTS - 1)

            @pl.when(s < n - 1)
            def _():
                to_mate(l, s + 1)

            convey(first_trip + s + 1, send_sums)
            return carry

        lax.fori_loop(1, n, step, 0)
        convey(jnp.int32(first_trip + n + 1))
        for d in range(2):
            for p in range(SUM_PARTS):
                rcopy(l, n - 1, d, p).wait_recv()
        pcopy(l, 0).wait_recv()
        new_h = (hacc[...] + (pcr[0] + rs[n])).astype(BF16)
        if l + 1 < layers:
            xb[l + 1, 0, mine] = new_h
        else:
            out[...] = new_h

        def drain(l):
            pcopy(l, n - 2).wait_send()
            pcopy(l, n - 1).wait_send()
            mcopy(l, 0).wait_send()
            if l == 0:
                cmcopy(0).wait_send()
            for d in range(2):
                for p in range(TOK_PARTS):
                    xcopy(l, 0, d, p).wait_send()
                if l == 0:
                    ccopy(0, d).wait_send()

            def one(s, carry):
                mcopy(l, s).wait_send()
                if l == 0:
                    cmcopy(s).wait_send()
                for d in range(2):
                    for p in range(SUM_PARTS):
                        rcopy(l, s, d, p).wait_send()

                @pl.when(s < n - 1)
                def _():
                    for d in range(2):
                        for p in range(TOK_PARTS):
                            xcopy(l, s, d, p).wait_send()
                        if l == 0:
                            ccopy(s, d).wait_send()
                return carry

            lax.fori_loop(1, n, one, 0)

    drain(layers - 1)
    for t in (trips - 2, trips - 1):
        for d in range(2):
            for h in range(MOVE_PARTS):
                ocopy(t, d, h).wait_send()
    for t in (units - 2, units - 1):
        vcopy(t).wait_send()

    def landed(t, carry):
        hcopy(t).wait_recv()
        return carry

    lax.fori_loop(0, trips, landed, 0)


def place_kernel(side, src, slot_to, hist, wg, wu, wd, og, ou, od, bg, bu, bd, rsem, wsem):
    layers, slots = wg.shape[:2]
    n = side * side
    per_layer = src.shape[0] // layers
    ff = hist.shape[-1]
    per_block = ff // 4 // piece_rows(ff)
    blocks = wg.shape[2] // (4 * per_block)
    me = lax.axis_index('ep')

    def place(dev):
        chip = lax.div(dev, 2)
        y, x = lax.div(chip, side), lax.rem(chip, side)
        turn = lax.rem(x + y, side)
        return side * y + turn, side * x + turn

    core = lax.rem(me, 2)
    at = place(me)
    groups = tuple(zip((wg, wu, wd), (bg, bu, bd), (og, ou, od)))
    for l in range(layers):
        for i in range(slots):
            here = me * slots + i
            moved = slot_to[l * per_layer] == here
            mv = l * per_layer
            for k in range(1, per_layer):
                hit = slot_to[l * per_layer + k] == here
                moved = moved | hit
                mv = jnp.where(hit, l * per_layer + k, mv)
            origin = place(lax.div(src[mv], slots))

            @pl.when(jnp.logical_not(moved))
            def _():
                for m, (w, buf, _) in enumerate(groups):
                    pltpu.make_async_copy(w.at[l, i], buf.at[l, i], rsem.at[l, i, m]).start()

            @pl.when(moved)
            def _():
                for which in range(2):
                    ring = core if which == 0 else 1 - core
                    gap = (at[0] - origin[0]) * (1 - ring) + (at[1] - origin[1]) * ring
                    for d in range(2):
                        away = lax.rem((gap if d == 0 else -gap) - 1 + 2 * n, n)
                        for m, (_, buf, _) in enumerate(groups):
                            for b in range(blocks):
                                first = away + (m * blocks + b) * per_block
                                come = hist.at[which, pl.ds(first, per_block), d, mv]
                                q = (2 * ring + d) * per_block
                                if m < 2:
                                    dst = buf.at[l, i, pl.ds(b * 4 * per_block + q, per_block)]
                                else:
                                    dst = buf.at[l, i, pl.ds(q, per_block), :, pl.ds(b * ff, ff)]
                                pltpu.make_async_copy(come, dst, rsem.at[l, i, m]).start()

    for l in range(layers):
        for i in range(slots):
            for m, (w, buf, o) in enumerate(groups):
                pltpu.make_async_copy(w.at[l, i], buf.at[l, i], rsem.at[l, i, m]).wait()
                pltpu.make_async_copy(buf.at[l, i], o.at[l, i], wsem.at[l, i, m]).start()
    for l in range(layers):
        for i in range(slots):
            for m, (w, buf, o) in enumerate(groups):
                pltpu.make_async_copy(buf.at[l, i], o.at[l, i], wsem.at[l, i, m]).wait()


def place_weights(src, slot_to, hist, weights, side):
    layers, slots = weights[0].shape[:2]
    SUB = piece_rows(weights[0].shape[3])
    split = [w.reshape(layers, slots, w.shape[2] // SUB, SUB, w.shape[3]) for w in weights]
    any_spec = pl.BlockSpec(memory_space=pl.ANY)
    smem = pl.BlockSpec(memory_space=pltpu.SMEM)
    out = pl.pallas_call(
        functools.partial(place_kernel, side),
        out_shape=[jax.ShapeDtypeStruct(w.shape, w.dtype) for w in split],
        in_specs=[smem, smem] + [any_spec] * 4,
        out_specs=[any_spec] * 3,
        scratch_shapes=[pltpu.VMEM(w.shape, w.dtype) for w in split] + [pltpu.SemaphoreType.DMA((layers, slots, 3))] * 2,
        compiler_params=pltpu.CompilerParams(vmem_limit_bytes=67043328),
        name='place_slots',
    )(src, slot_to, hist, *split)
    return tuple(o.reshape(w.shape) for o, w in zip(out, weights))


def moe(src, tok, coef, wg, wu, wd, sg, su, sd, group):
    layers, slots, dim, ff = wg.shape
    rows = tok.shape[0]
    sff = sg.shape[2]
    n = group // 2
    side = int(round(n ** 0.5))
    assert side * side * 2 == group
    dma = pltpu.SemaphoreType.DMA
    any_spec = pl.BlockSpec(memory_space=pl.ANY)
    vmem = pltpu.VMEM
    act_n = max(slots, -(-sff // ff))
    per_block, blocks, units = unit_counts(dim, ff)
    trips = units + n - 1
    moves = src.shape[0]
    assert layers * (n + 3) - 1 > trips + 1 and units > 2
    piece = (2, moves, piece_rows(ff), ff)
    scratch = [
        vmem((CELLS,) + piece, BF16),
        vmem((2,) + piece, BF16),
        vmem((2,) + piece, BF16),
        vmem((2,) + piece, BF16),
        vmem((layers, n, 2 * rows, dim), BF16),
        vmem((n, 2 * rows, coef.shape[1]), F32),
        vmem((layers, slots, dim, ff), BF16),
        vmem((layers, slots, dim, ff), BF16),
        vmem((layers, slots, ff, dim), BF16),
        vmem((dim, sff), BF16),
        vmem((dim, sff), BF16),
        vmem((sff, dim), BF16),
        vmem((act_n, 2 * rows, ff), BF16),
        vmem((rows, dim), F32),
        vmem((rows, dim), F32),
        vmem((2, rows, dim), F32),
        vmem((n, rows, dim), F32),
        vmem((n + 1, rows, dim), F32),
        dma((layers, 3)), dma((layers, 3)), dma((2,)),
        dma((layers, n, 2, TOK_PARTS)), dma((layers, n, 2, TOK_PARTS)),
        dma((layers, n)), dma((layers, n)),
        dma((n, 2)), dma((n, 2)),
        dma((n,)), dma((n,)),
        dma((2,)), dma((layers, n)),
        dma((layers, n, 2, SUM_PARTS)), dma((layers, n + 1, 2, SUM_PARTS)),
        dma((2, 2, MOVE_PARTS)), dma((CELLS, 2, MOVE_PARTS)), dma((2,)), dma((2,)), dma((trips,)), dma((2,)), dma((2,)),
        pltpu.SemaphoreType.REGULAR((2,)), pltpu.SemaphoreType.REGULAR,
        pltpu.SemaphoreType.REGULAR,
    ]
    flops = layers * 2 * 3 * dim * (ff * slots * rows * group + sff * rows)
    return pl.pallas_call(
        functools.partial(moe_kernel, side),
        out_shape=[jax.ShapeDtypeStruct((rows, dim), BF16), jax.ShapeDtypeStruct((2, trips) + piece, BF16)],
        in_specs=[pl.BlockSpec(memory_space=pltpu.SMEM)] + [any_spec] * 8,
        out_specs=[pl.BlockSpec(memory_space=pltpu.VMEM), any_spec],
        scratch_shapes=scratch,
        compiler_params=pltpu.CompilerParams(collective_id=0, has_side_effects=True, vmem_limit_bytes=67043328),
        cost_estimate=pl.CostEstimate(flops=flops * 4, bytes_accessed=40 << 20, transcendentals=0),
        name='moe_rings',
    )(src, tok, coef, wg, wu, wd, sg, su, sd)


def solution(mesh):
    group = mesh.shape['ep']

    def body(tok_in, routes, gate_vals, w_gate, w_up, w_down, sh_gate, sh_up, sh_down, old_map, move_slot, move_expert):
        layers = w_gate.shape[0]
        src = jnp.concatenate([first_holder(old_map[l], move_expert[l]) for l in range(layers)])
        coef = gate_table(routes, gate_vals, old_map)
        hidden, hist = moe(src, tok_in, coef, w_gate, w_up, w_down, sh_gate, sh_up, sh_down, group)
        side = int(round((group // 2) ** 0.5))
        new_w = place_weights(src, move_slot.reshape(-1), hist, (w_gate, w_up, w_down), side)
        return (hidden,) + new_w

    weight_spec = P(None, TOKEN_AXES, None, None)
    route_spec = P(None, TOKEN_AXES, None)
    map_spec = P(None, 'replica')
    shared_spec = P(None, None, None)
    tok_spec = P(TOKEN_AXES, None)
    return jax.shard_map(body, mesh=mesh, in_specs=(tok_spec, route_spec, route_spec, weight_spec, weight_spec, weight_spec, shared_spec, shared_spec, shared_spec, map_spec, map_spec, map_spec), out_specs=(tok_spec, weight_spec, weight_spec, weight_spec), check_vma=False)
```
